128 devices in a mesh: dp: 16 (over z, y_lo, core), tensor: 8 (over x, y_hi).
Axes of the slice: x: 4, y: 4 (y_hi: 2, y_lo: 2; y = y_hi * 2 + y_lo), z: 4, core: 2. Of those that a mesh axis runs over, the one named last changes fastest.
Arguments:
- requests: bfloat16 [1024, 8192], P('dp'), may hold values from -6 to 6
- base_gate_up_weight: bfloat16 [8192, 2, 28672], P('dp', None, 'tensor'), may hold values from -0.0625 to 0.0625
- adapter_down_weight: bfloat16 [128, 8192, 128], P('dp', 'tensor'), may hold values from -0.0625 to 0.0625
- adapter_up_weight: bfloat16 [128, 64, 2, 28672], P('dp', None, None, 'tensor'), may hold values from -0.75 to 0.75
- request_adapter: int32 [1024], P('dp'), may hold values from 0 to 127, as said below
- adapter_position: int32 [128], replicated, may hold values from 0 to 127, as said below
- counts: int32 [16], replicated, may hold values from 1 to 64, 768 in all
Outputs:
- hidden: bfloat16 [1024, 28672], P('dp', 'tensor')
The draws below stay inside these ranges and needn't reach their ends.
Inputs may be any that keep to these rules, and one draw needn't show every extreme that they name: `request_adapter`: the owner of store position s is s // 8. Among the 64 rows of one group at most 8 use adapters of one owner; in every draw one owner receives exactly 8 rows from every group. `adapter_position`: each store position appears once. `counts`: rows of a group past its count are padding.
All inputs are finite; a program needn't handle non-finite values.
Results may differ from the reference program's by a relative error of at most 0.0058.
Values may be sent and summed in bfloat16 or wider, within the bound.
A program may use at most 128 MiB of HBM per device.

```python
import math
import jax
import jax.numpy as jnp
import numpy as np
from jax import lax

MODEL_WIDTH = 8192
HIDDEN_UNITS = 28672
ADAPTER_RANK = 64
R = 64
PER_OWNER = 8
CAP = 8
ROWS = 1024
ADAPTER_TOTAL = 128
N_DP = 16


def adapter_table(key):
    return jax.random.permutation(jax.random.fold_in(key, 11), ADAPTER_TOTAL).astype(jnp.int32)


def draw_adapter_position(key, part):
    return adapter_table(key)


def draw_request_adapter(key, part):
    table = adapter_table(key)
    inverse = jnp.zeros((ADAPTER_TOTAL,), jnp.int32).at[table].set(jnp.arange(ADAPTER_TOTAL, dtype=jnp.int32))
    busiest = jax.random.randint(jax.random.fold_in(key, 12), (), 0, N_DP).astype(jnp.int32)
    total_slots = N_DP * CAP

    def one_group(index):
        sub = jax.random.fold_in(jax.random.fold_in(key, 13), index)
        order = jax.random.permutation(jax.random.fold_in(sub, 1), total_slots).astype(jnp.int32)
        owner = order // CAP
        ranking = jnp.where(owner == busiest, 0, 1) * total_slots + jnp.arange(total_slots, dtype=jnp.int32)
        picked = owner[jnp.argsort(ranking)][:R]
        mixed = jax.random.permutation(jax.random.fold_in(sub, 2), picked)
        local = jax.random.randint(jax.random.fold_in(sub, 3), (R,), 0, PER_OWNER).astype(jnp.int32)
        return inverse[mixed * PER_OWNER + local]
    return jax.vmap(one_group)(jnp.arange(N_DP, dtype=jnp.int32)).reshape(ROWS).astype(jnp.int32)


def level_of(key, dims, shards, smallest, top_value):
    loudness = 1.0
    for dim, shards_of in shards:
        steps = jax.random.uniform(jax.random.fold_in(jax.random.fold_in(key, 6), dim), (shards_of,), jnp.float32, smallest / len(shards), top_value / len(shards))
        loudness = loudness * jnp.repeat(jnp.exp(steps), dims[dim] // shards_of).reshape((-1,) + (1,) * (len(dims) - 1 - dim))
    return loudness


def length_profile(amount, total, limit, skew):
    weights = [(1 << 20) // math.isqrt(grade ** skew) + 1 for grade in range(2, amount + 1)]
    rest, holding = total - limit - (amount - 1), [1] * (amount - 1)
    while rest > 0:
        candidates = [i for i in range(amount - 1) if holding[i] < limit]
        mass, budget = sum([weights[i] for i in candidates]), rest
        for i in candidates:
            addition = min(limit - holding[i], max(1, budget * weights[i] // mass), rest)
            holding[i] = holding[i] + addition
            rest = rest - addition
    return np.array([limit] + holding)


def ragged(key, number_of, total, reach, slope):
    if number_of == 2:
        one = jax.random.randint(key, (), max(1, total - reach), min(reach, total - 1) + 1)
        return jnp.stack([one, total - one])
    sizes = jnp.asarray(length_profile(number_of, total, reach, slope), jnp.int32)
    couples = (number_of - 1) // 2
    source_of, sink = sizes[1:1 + 2 * couples:2], sizes[2:2 + 2 * couples:2]
    room = jnp.minimum(source_of - 1, reach - sink)
    passed = jax.random.randint(jax.random.fold_in(key, 1), (couples,), 0, 1 << 20) % (room + 1)
    sizes = sizes.at[1:1 + 2 * couples:2].set(source_of - passed).at[2:2 + 2 * couples:2].set(sink + passed)
    return sizes[jax.random.permutation(jax.random.fold_in(key, 2), number_of)]


def bell_draw(rng, dims, scale, bound, shards=(), kind=jnp.bfloat16):
    result = jax.random.normal(rng, dims, jnp.float32) * scale
    if len(shards) > 0:
        result = level_of(rng, dims, shards, -0.22, 0.18) * result
    return jnp.clip(result, min=-bound, max=bound).astype(kind)


def setup_inputs(seed: int = 0) -> dict:
    arg_keys = jax.random.split(jax.random.key(seed), 8)
    return {
        "requests": bell_draw(arg_keys[0], (ROWS, MODEL_WIDTH), 1.0, 6.0, ((0, 16),)),
        "base_gate_up_weight": bell_draw(arg_keys[1], (MODEL_WIDTH, 2, HIDDEN_UNITS), MODEL_WIDTH ** -0.5, 0.0625, ((0, 16), (2, 8))),
        "adapter_down_weight": bell_draw(arg_keys[2], (ADAPTER_TOTAL, MODEL_WIDTH, 2 * ADAPTER_RANK), MODEL_WIDTH ** -0.5, 0.0625, ((0, 16), (1, 8))),
        "adapter_up_weight": bell_draw(arg_keys[3], (ADAPTER_TOTAL, ADAPTER_RANK, 2, HIDDEN_UNITS), ADAPTER_RANK ** -0.5, 0.75, ((0, 16), (3, 8))),
        "request_adapter": draw_request_adapter(jax.random.fold_in(arg_keys[7], 71), 0),
        "adapter_position": draw_adapter_position(jax.random.fold_in(arg_keys[7], 71), 0),
        "counts": ragged(arg_keys[6], N_DP, 3 * R * N_DP // 4, R, 2).astype(jnp.int32),
    }


def reference(requests, base_gate_up_weight, adapter_down_weight, adapter_up_weight, request_adapter, adapter_position, counts):
    slot = adapter_position[request_adapter].astype(jnp.int32)

    def one_row(pair):
        row, store_location = pair
        down_matrix = lax.dynamic_index_in_dim(adapter_down_weight, store_location, 0, keepdims=False)
        down = jnp.dot(row[None, :], down_matrix, preferred_element_type=jnp.float32).astype(jnp.bfloat16)[0]
        up_matrix = lax.dynamic_index_in_dim(adapter_up_weight, store_location, 0, keepdims=False)
        term_gate = jnp.dot(down[None, :ADAPTER_RANK], up_matrix[:, 0, :], preferred_element_type=jnp.float32)[0]
        term_up = jnp.dot(down[None, ADAPTER_RANK:], up_matrix[:, 1, :], preferred_element_type=jnp.float32)[0]
        return jnp.stack([term_gate, term_up]).astype(jnp.bfloat16)

    delta = lax.map(one_row, (requests, slot), batch_size=16)
    gate = jnp.dot(requests, base_gate_up_weight[:, 0, :], preferred_element_type=jnp.float32) + delta[:, 0, :].astype(jnp.float32)
    up = jnp.dot(requests, base_gate_up_weight[:, 1, :], preferred_element_type=jnp.float32) + delta[:, 1, :].astype(jnp.float32)
    position = jnp.arange(ROWS, dtype=jnp.int32)
    live = (position % R) < counts[position // R]
    hidden = jnp.where(live[:, None], jax.nn.silu(gate) * up, 0.0)
    return hidden.astype(jnp.bfloat16)
```

```python
import functools

import jax
import jax.numpy as jnp
from jax import lax
from jax.experimental import pallas as pl
from jax.experimental.pallas import tpu as pltpu
from jax.sharding import PartitionSpec as P

MESH = pl.DeviceIdType.MESH
BF = jnp.bfloat16
F32 = jnp.float32
CHUNKS = 7
NA = 4
NB = 3


def remote(src, dst, send, recv, dp, tensor):
    return pltpu.make_async_remote_copy(
        src_ref=src, dst_ref=dst, send_sem=send, recv_sem=recv,
        device_id=(dp, tensor), device_id_type=MESH,
    )


def kernel(
    x, routed, wt, ut, ad, out,
    xe, we, uv, av, arr, dpart, rsr, dfull, rx, dl, part,
    a2s, a2r, a1s, a1r, ays, ayr, bys, byr, b2s, b2r, b1s, b1r, hs, hid,
    loc, ro_s, ro_r, x_s, x_r, xl_s, xl_r, w_s, w_r, t1_s, t1_r, t2_s, t2_r, rx_s, rx_r, dl_s, dl_r,
    a2_s, a2_q, a1_s, a1_q, ay_s, ay_q, by_s, by_q, b2_s, b2_q, b1_s, b1_q, h_s, h_q,
):
    d = lax.axis_index("dp")
    t = lax.axis_index("tensor")
    n_t = lax.axis_size("tensor")
    chip, c = lax.div(d, 2), lax.rem(d, 2)
    z, y = lax.div(chip, 2), lax.rem(chip, 2)
    yo = 1 - y
    mate = chip * 2 + 1 - c
    zp, zm, z2 = lax.rem(z + 1, 4), lax.rem(z + 3, 4), lax.rem(z + 2, 4)
    to_zp = (zp * 2 + y) * 2 + c
    to_zm = (zm * 2 + y) * 2 + c
    to_y = (z * 2 + yo) * 2 + c
    kc = xe.shape[1] - 256
    kh = kc // 2
    cw = we.shape[2]
    hw = cw // 2
    sub = rsr.shape[1]

    own_w = pltpu.make_async_copy(wt.at[c], we.at[:, pl.ds(c * kh, kh), :], loc.at[0])
    own_u = pltpu.make_async_copy(ut, uv, loc.at[1])
    own_a = pltpu.make_async_copy(ad, av, loc.at[2])
    own_r = pltpu.make_async_copy(routed.at[d], arr.at[d], loc.at[3])
    x_mine = x.at[:, pl.ds(pl.multiple_of(chip * kc, 128), kc)]
    x_rows = xe.at[pl.ds(d * 64, 64), pl.ds(0, kc)]
    own_x = pltpu.make_async_copy(x_mine, x_rows, loc.at[4])
    own_r.start()
    own_a.start()
    own_x.start()
    own_w.start()
    own_u.start()

    barrier = pltpu.get_barrier_semaphore()

    @pl.loop(1, 16)
    def _(i):
        pl.semaphore_signal(barrier, inc=1, device_id=(lax.rem(d + i, 16), t), device_id_type=MESH)

    @pl.loop(1, n_t)
    def _(i):
        pl.semaphore_signal(barrier, inc=1, device_id=(d, lax.rem(t + i, n_t)), device_id_type=MESH)

    pl.semaphore_wait(barrier, 15 + n_t - 1)

    def routed_copy(i):
        peer = lax.rem(d + i, 16)
        return remote(routed.at[peer], arr.at[d], ro_s.at[i], ro_r.at[i], peer, t)

    def x_copy(i):
        q = lax.rem(chip + i, 8)
        src = x.at[:, pl.ds(pl.multiple_of(q * kc, 128), kc)]
        return remote(src, x_rows, x_s.at[i], x_r.at[i], q * 2 + c, t)

    def x_relay(i):
        block = (lax.rem(chip + 8 - i, 8)) * 2 + c
        rows = xe.at[pl.ds(block * 64, 64), pl.ds(0, kc)]
        return remote(rows, rows, xl_s.at[i], xl_r.at[i], mate, t)

    @pl.loop(1, 16)
    def _(i):
        routed_copy(i).start()

    @pl.loop(1, 8)
    def _(i):
        x_copy(i).start()

    x_own_mate = remote(x_mine, x_rows, xl_s.at[0], xl_r.at[0], mate, t)
    x_own_mate.start()
    w_mate = remote(wt.at[1 - c], we.at[:, pl.ds(c * kh, kh), :], w_s, w_r, mate, t)
    w_mate.start()

    own_r.wait()
    own_a.wait()

    @pl.loop(1, 16)
    def _(i):
        routed_copy(i).wait_recv()

    kt = av.shape[1]
    rows_in = arr[...].astype(F32).reshape(128, kt + 128)
    body_in = rows_in[:, :kt].astype(BF)
    lab = rows_in[:, kt:]
    which = lab[:, 0:1].astype(jnp.int32)
    down = jnp.zeros((128, 128), F32)
    for a in range(8):
        term = jnp.dot(body_in, av[a], preferred_element_type=F32)
        down = down + jnp.where(which == a, term, 0.0)
    dpart[...] = down.reshape(n_t, sub, 128)

    def t1_copy(i):
        peer = lax.rem(t + i, n_t)
        return remote(dpart.at[peer], rsr.at[i], t1_s.at[i], t1_r.at[i], d, peer)

    def t2_copy(i):
        peer = lax.rem(t + i, n_t)
        return remote(dfull.at[t], dfull.at[t], t2_s.at[i], t2_r.at[i], d, peer)

    @pl.loop(1, n_t)
    def _(i):
        t1_copy(i).start()

    pick = (lax.broadcasted_iota(jnp.int32, (8, 128), 1) == 1).astype(BF)
    rx[c] = lax.dot_general(
        pick, lab.astype(BF), (((1,), (1,)), ((), ())), preferred_element_type=F32
    )
    rx_copy = remote(rx.at[c], rx.at[c], rx_s, rx_r, mate, t)
    rx_copy.start()

    total = dpart[t]

    @pl.loop(1, n_t)
    def _(i):
        t1_copy(i).wait_recv()

    for i in range(1, n_t):
        total = total + rsr[i]
    dfull[t] = total.astype(BF)

    @pl.loop(1, n_t)
    def _(i):
        t2_copy(i).start()

    @pl.loop(1, 8)
    def _(i):
        x_copy(i).wait_recv()
        x_relay(i).start()

    @pl.loop(1, n_t)
    def _(i):
        t2_copy(i).wait_recv()

    downs = dfull[...].astype(F32).reshape(128, 128).astype(BF)
    lane = lax.broadcasted_iota(jnp.int32, (128, 512), 1)
    src = lax.broadcasted_iota(jnp.int32, (128, 512), 0)
    mine = lax.div(lane, 64) == which

    def spread(offset):
        pattern = (src == lax.rem(lane, 64) + offset).astype(BF)
        copies = jnp.dot(downs, pattern, preferred_element_type=F32)
        return jnp.where(mine, copies, 0.0).astype(BF)

    wide_gate, wide_up = spread(0), spread(64)
    own_u.wait()
    for h in range(2):
        @pl.loop(0, CHUNKS)
        def _(j):
            dl[h, j, :, 0:hw] = jnp.dot(
                wide_gate, uv[h, j, :, 0:hw], preferred_element_type=F32
            ).astype(BF)
            dl[h, j, :, hw:cw] = jnp.dot(
                wide_up, uv[h, j, :, hw:cw], preferred_element_type=F32
            ).astype(BF)

    dl_copy = remote(
        dl.at[1 - c], we.at[:, pl.ds(kc + c * 128, 128), :], dl_s, dl_r, mate, t
    )
    dl_copy.start()

    @pl.loop(0, CHUNKS)
    def _(j):
        we[j, pl.ds(pl.multiple_of(kc + c * 128, 128), 128), :] = dl[c, j]

    rx_copy.wait_recv()
    for core in range(2):
        target = lax.broadcasted_iota(jnp.int32, (1024, 128), 1) // 8 * 64 + rx[core][0:1, :].astype(jnp.int32)
        hot = lax.broadcasted_iota(jnp.int32, (1024, 128), 0) == target
        xe[:, kc + core * 128 : kc + core * 128 + 128] = hot.astype(F32).astype(BF)

    own_x.wait()
    own_w.wait()
    x_own_mate.wait_recv()

    @pl.loop(1, 8)
    def _(i):
        x_relay(i).wait_recv()

    w_mate.wait_recv()
    dl_copy.wait_recv()

    def compute(k, first, count):
        @pl.loop(0, count)
        def _(i):
            zz = lax.rem(z + first + i, 4)
            rows = pl.ds(pl.multiple_of(zz * 256, 256), 256)
            part[k, rows, :] = jnp.dot(xe[rows, :], we[k], preferred_element_type=F32)

    def rows_of(zz, yy):
        return pl.ds(pl.multiple_of(zz * 256 + yy * 128, 128), 128)

    def half_of(zz, yy, cc):
        return pl.ds(pl.multiple_of(zz * 256 + yy * 128 + cc * 64, 64), 64)

    def ra2(s, w):
        return remote(a2s.at[s, w], a2r.at[s, w], a2_s.at[s, w], a2_q.at[s, w], (to_zp, to_zm)[w], t)

    def ra1(s, w, p):
        return remote(a1s.at[s, w, p], a1r.at[s, w, p], a1_s.at[s, w, p], a1_q.at[s, w, p], (to_zp, to_zm)[w], t)

    def ray(s):
        return remote(ays.at[s], ayr.at[s], ay_s.at[s], ay_q.at[s], to_y, t)

    def rby(s, i):
        return remote(bys.at[s, i], byr.at[s, i], by_s.at[s, i], by_q.at[s, i], to_y, t)

    def rb2(s, w):
        return remote(b2s.at[s, w], b2r.at[s, w], b2_s.at[s, w], b2_q.at[s, w], (to_zp, to_zm)[w], t)

    def rb1(s, w, p):
        return remote(b1s.at[s, w, p], b1r.at[s, w, p], b1_s.at[s, w, p], b1_q.at[s, w, p], (to_zp, to_zm)[w], t)

    def rh(k):
        return remote(
            hs.at[k, 1 - c], hid.at[c, :, pl.ds(pl.multiple_of(k * hw, 128), hw)],
            h_s.at[k], h_q.at[k], mate, t,
        )

    def a_first(s):
        k = 2 * s
        compute(k, 1, 3)
        a2s[s, 0] = part[k, rows_of(z2, 0), :].astype(BF)
        ra2(s, 0).start()
        a2s[s, 1] = part[k, rows_of(z2, 1), :].astype(BF)
        ra2(s, 1).start()
        a1s[s, 0, 1] = part[k, rows_of(zp, 1), :].astype(BF)
        ra1(s, 0, 1).start()
        a1s[s, 1, 1] = part[k, rows_of(zm, 0), :].astype(BF)
        ra1(s, 1, 1).start()

    def a_pass(s):
        k = 2 * s
        for w, zz in ((0, zp), (1, zm)):
            ra2(s, w).wait_recv()
            a1s[s, w, 0] = (part[k, rows_of(zz, w), :] + a2r[s, w].astype(F32)).astype(BF)
            ra1(s, w, 0).start()

    def a_cross(s):
        k = 2 * s
        compute(k, 0, 1)
        for w in range(2):
            for p in range(2):
                ra1(s, w, p).wait_recv()
        ays[s] = (
            part[k, rows_of(z, yo), :] + a1r[s, yo, 0].astype(F32) + a1r[s, y, 1].astype(F32)
        ).astype(BF)
        ray(s).start()
        part[k, rows_of(z, y), :] = (
            part[k, rows_of(z, y), :] + a1r[s, y, 0].astype(F32) + a1r[s, yo, 1].astype(F32)
        )

    def finish(k, cc, total):
        gate, up = total[:, :hw], total[:, hw:]
        hs[k, cc] = (gate / (1.0 + jnp.exp(-gate)) * up).astype(BF)

    def deliver(k):
        rh(k).start()
        hid[c, :, pl.ds(pl.multiple_of(k * hw, 128), hw)] = hs[k, c]

    def a_last(s):
        k = 2 * s
        ray(s).wait_recv()
        for cc in range(2):
            finish(k, cc, part[k, half_of(z, y, cc), :] + ayr[s, cc * 64 : cc * 64 + 64, :].astype(F32))
        deliver(k)

    def b_first(s):
        k = 2 * s + 1
        compute(k, 0, 4)
        for i in (2, 1, 3, 0):
            zz = lax.rem(z + i, 4)
            bys[s, i] = part[k, rows_of(zz, yo), :].astype(BF)
            rby(s, i).start()

    def b_second(s):
        k = 2 * s + 1
        rby(s, 2).wait_recv()
        for cc in range(2):
            b2s[s, cc] = (
                part[k, half_of(z2, y, cc), :] + byr[s, 2, cc * 64 : cc * 64 + 64, :].astype(F32)
            ).astype(BF)
            rb2(s, cc).start()
        for w, zz, i in ((0, zp, 1), (1, zm, 3)):
            rby(s, i).wait_recv()
            o = 1 - w
            b1s[s, w, 1] = (
                part[k, half_of(zz, y, o), :] + byr[s, i, o * 64 : o * 64 + 64, :].astype(F32)
            ).astype(BF)
            rb1(s, w, 1).start()

    def b_pass(s):
        k = 2 * s + 1
        for w, zz, i in ((0, zp, 1), (1, zm, 3)):
            rb2(s, w).wait_recv()
            b1s[s, w, 0] = (
                part[k, half_of(zz, y, w), :]
                + byr[s, i, w * 64 : w * 64 + 64, :].astype(F32)
                + b2r[s, w].astype(F32)
            ).astype(BF)
            rb1(s, w, 0).start()

    def b_last(s):
        k = 2 * s + 1
        rby(s, 0).wait_recv()
        for w in range(2):
            for p in range(2):
                rb1(s, w, p).wait_recv()
        for cc in range(2):
            finish(
                k, cc,
                part[k, half_of(z, y, cc), :]
                + byr[s, 0, cc * 64 : cc * 64 + 64, :].astype(F32)
                + b1r[s, cc, 0].astype(F32)
                + b1r[s, 1 - cc, 1].astype(F32),
            )
        deliver(k)

    @pl.loop(0, NA)
    def _(s):
        a_first(s)

        @pl.when(s < NB)
        def _():
            b_first(s)

    @pl.loop(0, NA)
    def _(s):
        a_pass(s)

    @pl.loop(0, NA)
    def _(s):
        a_cross(s)

        @pl.when(s < NB)
        def _():
            b_second(s)

    @pl.loop(0, NB)
    def _(s):
        b_pass(s)

    @pl.loop(0, NA)
    def _(s):
        a_last(s)

    @pl.loop(0, NB)
    def _(s):
        b_last(s)

    @pl.loop(0, CHUNKS)
    def _(k):
        rh(k).wait_recv()

    half = hw * CHUNKS
    out[:, 0:half] = hid[0]
    out[:, half : 2 * half] = hid[1]

    @pl.loop(1, 16)
    def _(i):
        routed_copy(i).wait_send()

    @pl.loop(1, 8)
    def _(i):
        x_copy(i).wait_send()
        x_relay(i).wait_send()

    x_own_mate.wait_send()
    w_mate.wait_send()
    rx_copy.wait_send()
    dl_copy.wait_send()

    @pl.loop(1, n_t)
    def _(i):
        t1_copy(i).wait_send()
        t2_copy(i).wait_send()

    @pl.loop(0, NA)
    def _(s):
        ray(s).wait_send()
        for w in range(2):
            ra2(s, w).wait_send()
            for p in range(2):
                ra1(s, w, p).wait_send()

    @pl.loop(0, NB)
    def _(s):
        for i in range(4):
            rby(s, i).wait_send()
        for w in range(2):
            rb2(s, w).wait_send()
            for p in range(2):
                rb1(s, w, p).wait_send()

    @pl.loop(0, CHUNKS)
    def _(k):
        rh(k).wait_send()


def halves(weight, depth, units):
    hw = units // (2 * CHUNKS)
    cut = weight.reshape(depth, 2, 2, CHUNKS, hw)
    return jnp.transpose(cut, (2, 3, 0, 1, 4)).reshape(2, CHUNKS, depth, 2 * hw)


def body(requests, base, adown, aup, request_adapter, adapter_position, counts):
    rows, width = requests.shape
    n_t = lax.axis_size("tensor")
    group, lane = lax.axis_index("dp"), lax.axis_index("tensor")
    units = base.shape[2]
    per_owner, kt, rank2 = adown.shape
    capacity = 8
    slots = 16 * capacity
    match = (
        request_adapter[:, None] == jnp.arange(adapter_position.shape[0], dtype=jnp.int32)[None, :]
    )
    slot = jnp.sum(jnp.where(match, adapter_position[None, :], 0), axis=1)
    owner = slot // per_owner
    local = slot % per_owner
    owner_hot = (owner[:, None] == jnp.arange(16, dtype=jnp.int32)[None, :]).astype(jnp.int32)
    place = jnp.sum(owner_hot * (jnp.cumsum(owner_hot, axis=0) - 1), axis=1)
    target = owner * capacity + place
    select = (target[None, :] == jnp.arange(slots, dtype=jnp.int32)[:, None]).astype(BF)
    piece = lax.dynamic_slice_in_dim(requests, lane * kt, kt, 1)
    row_index = jnp.arange(rows, dtype=jnp.int32)
    lanes = jnp.arange(128, dtype=jnp.int32)[None, :]
    labels = jnp.where(
        lanes == 0, local[:, None], jnp.where(lanes == 1, row_index[:, None], 0)
    ).astype(BF)
    routed = jnp.dot(
        select, jnp.concatenate([piece, labels], axis=1), preferred_element_type=F32
    ).astype(BF).reshape(16, capacity, kt + 128)

    wt = halves(base, base.shape[0], units)
    ut = halves(aup, aup.shape[0] * aup.shape[1], units)
    kc = width // 8
    hw = units // (2 * CHUNKS)
    cw = 2 * hw
    sub = 128 // n_t
    vm, dma = pltpu.VMEM, pltpu.SemaphoreType.DMA
    both = [
        vm((NA, 2, 128, cw), BF), vm((NA, 2, 128, cw), BF),
        vm((NA, 2, 2, 128, cw), BF), vm((NA, 2, 2, 128, cw), BF),
        vm((NA, 128, cw), BF), vm((NA, 128, cw), BF),
        vm((NB, 4, 128, cw), BF), vm((NB, 4, 128, cw), BF),
        vm((NB, 2, 64, cw), BF), vm((NB, 2, 64, cw), BF),
        vm((NB, 2, 2, 64, cw), BF), vm((NB, 2, 2, 64, cw), BF),
        vm((CHUNKS, 2, 64, hw), BF), vm((2, 64, hw * CHUNKS), BF),
    ]
    sems = [
        dma((5,)), dma((16,)), dma((16,)), dma((8,)), dma((8,)), dma((8,)), dma((8,)),
        dma, dma, dma((n_t,)), dma((n_t,)), dma((n_t,)), dma((n_t,)), dma, dma, dma, dma,
        dma((NA, 2)), dma((NA, 2)), dma((NA, 2, 2)), dma((NA, 2, 2)), dma((NA,)), dma((NA,)),
        dma((NB, 4)), dma((NB, 4)), dma((NB, 2)), dma((NB, 2)), dma((NB, 2, 2)), dma((NB, 2, 2)),
        dma((CHUNKS,)), dma((CHUNKS,)),
    ]
    hidden = pl.pallas_call(
        kernel,
        out_shape=jax.ShapeDtypeStruct((rows, units), BF),
        in_specs=[pl.BlockSpec(memory_space=pl.ANY)] * 5,
        out_specs=pl.BlockSpec(memory_space=pltpu.VMEM),
        scratch_shapes=[
            vm((16 * rows, kc + 256), BF), vm((CHUNKS, kc + 256, cw), BF),
            vm(ut.shape, BF), vm(adown.shape, BF), vm((16, capacity, kt + 128), BF),
            vm((n_t, sub, 128), F32), vm((n_t, sub, 128), F32), vm((n_t, sub, 128), BF),
            vm((2, 8, 128), F32), vm((2, CHUNKS, 128, cw), BF), vm((CHUNKS, 16 * rows, cw), F32),
        ] + both + sems,
        compiler_params=pltpu.CompilerParams(
            collective_id=0, has_side_effects=True, vmem_limit_bytes=67043328
        ),
    )(requests, routed, wt, ut, adown)
    live = row_index < counts[group]
    return jnp.where(live[:, None], hidden, jnp.zeros_like(hidden))


def solution(mesh):
    placed = (
        P("dp", None),
        P("dp", None, "tensor"),
        P("dp", "tensor", None),
        P("dp", None, None, "tensor"),
        P("dp"),
        P(),
        P(),
    )
    return jax.shard_map(
        body, mesh=mesh, in_specs=placed, out_specs=P("dp", "tensor"), check_vma=False
    )
```

```python
import functools

import jax
import jax.numpy as jnp
from jax import lax
from jax.experimental import pallas as pl
from jax.experimental.pallas import tpu as pltpu
from jax.sharding import PartitionSpec as P

MESH = pl.DeviceIdType.MESH
BF = jnp.bfloat16
F32 = jnp.float32
CHUNKS = 7
NA = 4
NB = 3


def remote(src, dst, send, recv, dp, tensor):
    return pltpu.make_async_remote_copy(
        src_ref=src, dst_ref=dst, send_sem=send, recv_sem=recv,
        device_id=(dp, tensor), device_id_type=MESH,
    )


def kernel(
    x, routed, wt, ut, ad, out,
    xe, we, wr, ur, av, arr, dpart, rsr, dfull, rx, dl, part,
    a2s, a2r, a1s, a1r, ays, ayr, bys, byr, b2s, b2r, b1s, b1r, hs, hid,
    loc, ro_s, ro_r, x_s, x_r, xl_s, xl_r, w_s, w_r, t1_s, t1_r, t2_s, t2_r, rx_s, rx_r, dl_s, dl_r,
    a2_s, a2_q, a1_s, a1_q, ay_s, ay_q, by_s, by_q, b2_s, b2_q, b1_s, b1_q, h_s, h_q,
):
    d = lax.axis_index("dp")
    t = lax.axis_index("tensor")
    n_t = lax.axis_size("tensor")
    chip, c = lax.div(d, 2), lax.rem(d, 2)
    z, y = lax.div(chip, 2), lax.rem(chip, 2)
    yo = 1 - y
    mate = chip * 2 + 1 - c
    zp, zm, z2 = lax.rem(z + 1, 4), lax.rem(z + 3, 4), lax.rem(z + 2, 4)
    to_zp = (zp * 2 + y) * 2 + c
    to_zm = (zm * 2 + y) * 2 + c
    to_y = (z * 2 + yo) * 2 + c
    kc = xe.shape[1] - 256
    kh = kc // 2
    cw = we.shape[2]
    hw = cw // 2
    sub = rsr.shape[1]

    half = hw * CHUNKS

    def units(h):
        return pl.ds(pl.multiple_of(h * half, 128), half)

    w_rows = wr.at[pl.ds(c * kh, kh)]
    own_w = pltpu.make_async_copy(wt.at[:, :, units(c)], w_rows, loc.at[0])
    own_u = pltpu.make_async_copy(ut, ur, loc.at[1])
    own_a = pltpu.make_async_copy(ad, av, loc.at[2])
    own_r = pltpu.make_async_copy(routed.at[d], arr.at[d], loc.at[3])
    x_mine = x.at[:, pl.ds(pl.multiple_of(chip * kc, 128), kc)]
    x_rows = xe.at[pl.ds(d * 64, 64), pl.ds(0, kc)]
    own_x = pltpu.make_async_copy(x_mine, x_rows, loc.at[4])
    own_r.start()
    own_a.start()
    own_x.start()
    own_w.start()
    own_u.start()

    barrier = pltpu.get_barrier_semaphore()

    @pl.loop(1, 16)
    def _(i):
        pl.semaphore_signal(barrier, inc=1, device_id=(lax.rem(d + i, 16), t), device_id_type=MESH)

    @pl.loop(1, n_t)
    def _(i):
        pl.semaphore_signal(barrier, inc=1, device_id=(d, lax.rem(t + i, n_t)), device_id_type=MESH)

    pl.semaphore_wait(barrier, 15 + n_t - 1)

    def routed_copy(i):
        peer = lax.rem(d + i, 16)
        return remote(routed.at[peer], arr.at[d], ro_s.at[i], ro_r.at[i], peer, t)

    def x_copy(i):
        q = lax.rem(chip + i, 8)
        src = x.at[:, pl.ds(pl.multiple_of(q * kc, 128), kc)]
        return remote(src, x_rows, x_s.at[i], x_r.at[i], q * 2 + c, t)

    def x_relay(i):
        block = (lax.rem(chip + 8 - i, 8)) * 2 + c
        rows = xe.at[pl.ds(block * 64, 64), pl.ds(0, kc)]
        return remote(rows, rows, xl_s.at[i], xl_r.at[i], mate, t)

    @pl.loop(1, 16)
    def _(i):
        routed_copy(i).start()

    @pl.loop(1, 8)
    def _(i):
        x_copy(i).start()

    x_own_mate = remote(x_mine, x_rows, xl_s.at[0], xl_r.at[0], mate, t)
    x_own_mate.start()
    w_mate = remote(wt.at[:, :, units(1 - c)], w_rows, w_s, w_r, mate, t)
    w_mate.start()

    to = lax.broadcasted_iota(jnp.int32, (256, 256), 0)
    at = lax.broadcasted_iota(jnp.int32, (256, 256), 1)
    parting = (at == lax.rem(to, 128) * 2 + lax.div(to, 128)).astype(F32).astype(BF)
    blocks = kh // 128

    def part_weight(owner):
        @pl.loop(0, blocks)
        def _(i):
            b = owner * blocks + i
            rows = pl.ds(pl.multiple_of(b * 128, 128), 128)
            for j in range(CHUNKS):
                pairs = wr[rows, :, j * hw : j * hw + hw].reshape(256, hw)
                parted = jnp.dot(parting, pairs, preferred_element_type=F32).astype(BF)
                we[j, rows, 0:hw] = parted[0:128]
                we[j, rows, hw:cw] = parted[128:256]

    own_w.wait()
    part_weight(c)

    own_r.wait()
    own_a.wait()

    @pl.loop(1, 16)
    def _(i):
        routed_copy(i).wait_recv()

    kt = av.shape[1]
    rows_in = arr[...].astype(F32).reshape(128, kt + 128)
    body_in = rows_in[:, :kt].astype(BF)
    lab = rows_in[:, kt:]
    which = lab[:, 0:1].astype(jnp.int32)
    down = jnp.zeros((128, 128), F32)
    for a in range(8):
        term = jnp.dot(body_in, av[a], preferred_element_type=F32)
        down = down + jnp.where(which == a, term, 0.0)
    dpart[...] = down.reshape(n_t, sub, 128)

    def t1_copy(i):
        peer = lax.rem(t + i, n_t)
        return remote(dpart.at[peer], rsr.at[i], t1_s.at[i], t1_r.at[i], d, peer)

    def t2_copy(i):
        peer = lax.rem(t + i, n_t)
        return remote(dfull.at[t], dfull.at[t], t2_s.at[i], t2_r.at[i], d, peer)

    @pl.loop(1, n_t)
    def _(i):
        t1_copy(i).start()

    pick = (lax.broadcasted_iota(jnp.int32, (8, 128), 1) == 1).astype(BF)
    rx[c] = lax.dot_general(
        pick, lab.astype(BF), (((1,), (1,)), ((), ())), preferred_element_type=F32
    )
    rx_copy = remote(rx.at[c], rx.at[c], rx_s, rx_r, mate, t)
    rx_copy.start()

    total = dpart[t]

    @pl.loop(1, n_t)
    def _(i):
        t1_copy(i).wait_recv()

    for i in range(1, n_t):
        total = total + rsr[i]
    dfull[t] = total.astype(BF)

    @pl.loop(1, n_t)
    def _(i):
        t2_copy(i).start()

    @pl.loop(1, 8)
    def _(i):
        x_copy(i).wait_recv()
        x_relay(i).start()

    @pl.loop(1, n_t)
    def _(i):
        t2_copy(i).wait_recv()

    downs = dfull[...].astype(F32).reshape(128, 128).astype(BF)
    deep = 2 * ur.shape[0]
    lane = lax.broadcasted_iota(jnp.int32, (128, deep), 1)
    src = lax.broadcasted_iota(jnp.int32, (128, deep), 0)
    mine = lax.div(lane, 128) == which
    rank = lax.div(lax.rem(lane, 128), 2)

    def spread(which_term):
        pattern = (src == rank + 64 * which_term).astype(F32).astype(BF)
        copies = jnp.dot(downs, pattern, preferred_element_type=F32)
        return jnp.where(mine & (lax.rem(lane, 2) == which_term), copies, 0.0).astype(BF)

    wide = jnp.concatenate([spread(0), spread(1)], axis=0)
    own_u.wait()
    for h in range(2):
        @pl.loop(0, CHUNKS)
        def _(j):
            cols = pl.ds(pl.multiple_of(h * half + j * hw, 128), hw)
            both = jnp.dot(
                wide, ur[:, :, cols].reshape(deep, hw), preferred_element_type=F32
            ).astype(BF)
            dl[h, j, :, 0:hw] = both[0:128]
            dl[h, j, :, hw:cw] = both[128:256]

    dl_copy = remote(
        dl.at[1 - c], we.at[:, pl.ds(kc + c * 128, 128), :], dl_s, dl_r, mate, t
    )
    dl_copy.start()

    @pl.loop(0, CHUNKS)
    def _(j):
        we[j, pl.ds(pl.multiple_of(kc + c * 128, 128), 128), :] = dl[c, j]

    w_mate.wait_recv()
    part_weight(1 - c)
    rx_copy.wait_recv()
    for core in range(2):
        target = lax.broadcasted_iota(jnp.int32, (1024, 128), 1) // 8 * 64 + rx[core][0:1, :].astype(jnp.int32)
        hot = lax.broadcasted_iota(jnp.int32, (1024, 128), 0) == target
        xe[:, kc + core * 128 : kc + core * 128 + 128] = hot.astype(F32).astype(BF)

    own_x.wait()
    x_own_mate.wait_recv()

    @pl.loop(1, 8)
    def _(i):
        x_relay(i).wait_recv()

    dl_copy.wait_recv()

    def compute(k, first, count):
        @pl.loop(0, count)
        def _(i):
            zz = lax.rem(z + first + i, 4)
            rows = pl.ds(pl.multiple_of(zz * 256, 256), 256)
            part[k, rows, :] = jnp.dot(xe[rows, :], we[k], preferred_element_type=F32)

    def rows_of(zz, yy):
        return pl.ds(pl.multiple_of(zz * 256 + yy * 128, 128), 128)

    def half_of(zz, yy, cc):
        return pl.ds(pl.multiple_of(zz * 256 + yy * 128 + cc * 64, 64), 64)

    def ra2(s, w):
        return remote(a2s.at[s, w], a2r.at[s, w], a2_s.at[s, w], a2_q.at[s, w], (to_zp, to_zm)[w], t)

    def ra1(s, w, p):
        return remote(a1s.at[s, w, p], a1r.at[s, w, p], a1_s.at[s, w, p], a1_q.at[s, w, p], (to_zp, to_zm)[w], t)

    def ray(s):
        return remote(ays.at[s], ayr.at[s], ay_s.at[s], ay_q.at[s], to_y, t)

    def rby(s, i):
        return remote(bys.at[s, i], byr.at[s, i], by_s.at[s, i], by_q.at[s, i], to_y, t)

    def rb2(s, w):
        return remote(b2s.at[s, w], b2r.at[s, w], b2_s.at[s, w], b2_q.at[s, w], (to_zp, to_zm)[w], t)

    def rb1(s, w, p):
        return remote(b1s.at[s, w, p], b1r.at[s, w, p], b1_s.at[s, w, p], b1_q.at[s, w, p], (to_zp, to_zm)[w], t)

    def rh(k):
        return remote(
            hs.at[k, 1 - c], hid.at[c, :, pl.ds(pl.multiple_of(k * hw, 128), hw)],
            h_s.at[k], h_q.at[k], mate, t,
        )

    def a_first(s):
        k = 2 * s
        compute(k, 1, 3)
        a2s[s, 0] = part[k, rows_of(z2, 0), :].astype(BF)
        ra2(s, 0).start()
        a2s[s, 1] = part[k, rows_of(z2, 1), :].astype(BF)
        ra2(s, 1).start()
        a1s[s, 0, 1] = part[k, rows_of(zp, 1), :].astype(BF)
        ra1(s, 0, 1).start()
        a1s[s, 1, 1] = part[k, rows_of(zm, 0), :].astype(BF)
        ra1(s, 1, 1).start()

    def a_pass(s):
        k = 2 * s
        for w, zz in ((0, zp), (1, zm)):
            ra2(s, w).wait_recv()
            a1s[s, w, 0] = (part[k, rows_of(zz, w), :] + a2r[s, w].astype(F32)).astype(BF)
            ra1(s, w, 0).start()

    def a_cross(s):
        k = 2 * s
        compute(k, 0, 1)
        for w in range(2):
            for p in range(2):
                ra1(s, w, p).wait_recv()
        ays[s] = (
            part[k, rows_of(z, yo), :] + a1r[s, yo, 0].astype(F32) + a1r[s, y, 1].astype(F32)
        ).astype(BF)
        ray(s).start()
        part[k, rows_of(z, y), :] = (
            part[k, rows_of(z, y), :] + a1r[s, y, 0].astype(F32) + a1r[s, yo, 1].astype(F32)
        )

    def finish(k, cc, total):
        gate, up = total[:, :hw], total[:, hw:]
        hs[k, cc] = (gate / (1.0 + jnp.exp(-gate)) * up).astype(BF)

    def deliver(k):
        rh(k).start()
        hid[c, :, pl.ds(pl.multiple_of(k * hw, 128), hw)] = hs[k, c]

    def a_last(s):
        k = 2 * s
        ray(s).wait_recv()
        for cc in range(2):
            finish(k, cc, part[k, half_of(z, y, cc), :] + ayr[s, cc * 64 : cc * 64 + 64, :].astype(F32))
        deliver(k)

    def b_first(s):
        k = 2 * s + 1
        compute(k, 0, 4)
        for i in (2, 1, 3, 0):
            zz = lax.rem(z + i, 4)
            bys[s, i] = part[k, rows_of(zz, yo), :].astype(BF)
            rby(s, i).start()

    def b_second(s):
        k = 2 * s + 1
        rby(s, 2).wait_recv()
        for cc in range(2):
            b2s[s, cc] = (
                part[k, half_of(z2, y, cc), :] + byr[s, 2, cc * 64 : cc * 64 + 64, :].astype(F32)
            ).astype(BF)
            rb2(s, cc).start()
        for w, zz, i in ((0, zp, 1), (1, zm, 3)):
            rby(s, i).wait_recv()
            o = 1 - w
            b1s[s, w, 1] = (
                part[k, half_of(zz, y, o), :] + byr[s, i, o * 64 : o * 64 + 64, :].astype(F32)
            ).astype(BF)
            rb1(s, w, 1).start()

    def b_pass(s):
        k = 2 * s + 1
        for w, zz, i in ((0, zp, 1), (1, zm, 3)):
            rb2(s, w).wait_recv()
            b1s[s, w, 0] = (
                part[k, half_of(zz, y, w), :]
                + byr[s, i, w * 64 : w * 64 + 64, :].astype(F32)
                + b2r[s, w].astype(F32)
            ).astype(BF)
            rb1(s, w, 0).start()

    def b_last(s):
        k = 2 * s + 1
        rby(s, 0).wait_recv()
        for w in range(2):
            for p in range(2):
                rb1(s, w, p).wait_recv()
        for cc in range(2):
            finish(
                k, cc,
                part[k, half_of(z, y, cc), :]
                + byr[s, 0, cc * 64 : cc * 64 + 64, :].astype(F32)
                + b1r[s, cc, 0].astype(F32)
                + b1r[s, 1 - cc, 1].astype(F32),
            )
        deliver(k)

    @pl.loop(0, NA)
    def _(s):
        a_first(s)

        @pl.when(s < NB)
        def _():
            b_first(s)

    @pl.loop(0, NA)
    def _(s):
        a_pass(s)

    @pl.loop(0, NA)
    def _(s):
        a_cross(s)

        @pl.when(s < NB)
        def _():
            b_second(s)

    @pl.loop(0, NB)
    def _(s):
        b_pass(s)

    @pl.loop(0, NA)
    def _(s):
        a_last(s)

    @pl.loop(0, NB)
    def _(s):
        b_last(s)

    @pl.loop(0, CHUNKS)
    def _(k):
        rh(k).wait_recv()

    out[:, 0:half] = hid[0]
    out[:, half : 2 * half] = hid[1]

    @pl.loop(1, 16)
    def _(i):
        routed_copy(i).wait_send()

    @pl.loop(1, 8)
    def _(i):
        x_copy(i).wait_send()
        x_relay(i).wait_send()

    x_own_mate.wait_send()
    w_mate.wait_send()
    rx_copy.wait_send()
    dl_copy.wait_send()

    @pl.loop(1, n_t)
    def _(i):
        t1_copy(i).wait_send()
        t2_copy(i).wait_send()

    @pl.loop(0, NA)
    def _(s):
        ray(s).wait_send()
        for w in range(2):
            ra2(s, w).wait_send()
            for p in range(2):
                ra1(s, w, p).wait_send()

    @pl.loop(0, NB)
    def _(s):
        for i in range(4):
            rby(s, i).wait_send()
        for w in range(2):
            rb2(s, w).wait_send()
            for p in range(2):
                rb1(s, w, p).wait_send()

    @pl.loop(0, CHUNKS)
    def _(k):
        rh(k).wait_send()


def body(requests, base, adown, aup, request_adapter, adapter_position, counts):
    rows, width = requests.shape
    n_t = lax.axis_size("tensor")
    group, lane = lax.axis_index("dp"), lax.axis_index("tensor")
    units = base.shape[2]
    per_owner, kt, rank2 = adown.shape
    capacity = 8
    slots = 16 * capacity
    match = (
        request_adapter[:, None] == jnp.arange(adapter_position.shape[0], dtype=jnp.int32)[None, :]
    )
    slot = jnp.sum(jnp.where(match, adapter_position[None, :], 0), axis=1)
    owner = slot // per_owner
    local = slot % per_owner
    owner_hot = (owner[:, None] == jnp.arange(16, dtype=jnp.int32)[None, :]).astype(jnp.int32)
    place = jnp.sum(owner_hot * (jnp.cumsum(owner_hot, axis=0) - 1), axis=1)
    target = owner * capacity + place
    select = (target[None, :] == jnp.arange(slots, dtype=jnp.int32)[:, None]).astype(BF)
    piece = lax.dynamic_slice_in_dim(requests, lane * kt, kt, 1)
    row_index = jnp.arange(rows, dtype=jnp.int32)
    lanes = jnp.arange(128, dtype=jnp.int32)[None, :]
    labels = jnp.where(
        lanes == 0, local[:, None], jnp.where(lanes == 1, row_index[:, None], 0)
    ).astype(BF)
    routed = jnp.dot(
        select, jnp.concatenate([piece, labels], axis=1), preferred_element_type=F32
    ).astype(BF).reshape(16, capacity, kt + 128)

    ut = aup.reshape(aup.shape[0] * aup.shape[1], 2, units)
    kc = width // 8
    hw = units // (2 * CHUNKS)
    cw = 2 * hw
    sub = 128 // n_t
    vm, dma = pltpu.VMEM, pltpu.SemaphoreType.DMA
    both = [
        vm((NA, 2, 128, cw), BF), vm((NA, 2, 128, cw), BF),
        vm((NA, 2, 2, 128, cw), BF), vm((NA, 2, 2, 128, cw), BF),
        vm((NA, 128, cw), BF), vm((NA, 128, cw), BF),
        vm((NB, 4, 128, cw), BF), vm((NB, 4, 128, cw), BF),
        vm((NB, 2, 64, cw), BF), vm((NB, 2, 64, cw), BF),
        vm((NB, 2, 2, 64, cw), BF), vm((NB, 2, 2, 64, cw), BF),
        vm((CHUNKS, 2, 64, hw), BF), vm((2, 64, hw * CHUNKS), BF),
    ]
    sems = [
        dma((5,)), dma((16,)), dma((16,)), dma((8,)), dma((8,)), dma((8,)), dma((8,)),
        dma, dma, dma((n_t,)), dma((n_t,)), dma((n_t,)), dma((n_t,)), dma, dma, dma, dma,
        dma((NA, 2)), dma((NA, 2)), dma((NA, 2, 2)), dma((NA, 2, 2)), dma((NA,)), dma((NA,)),
        dma((NB, 4)), dma((NB, 4)), dma((NB, 2)), dma((NB, 2)), dma((NB, 2, 2)), dma((NB, 2, 2)),
        dma((CHUNKS,)), dma((CHUNKS,)),
    ]
    hidden = pl.pallas_call(
        kernel,
        out_shape=jax.ShapeDtypeStruct((rows, units), BF),
        in_specs=[pl.BlockSpec(memory_space=pl.ANY)] * 5,
        out_specs=pl.BlockSpec(memory_space=pltpu.VMEM),
        scratch_shapes=[
            vm((16 * rows, kc + 256), BF), vm((CHUNKS, kc + 256, cw), BF),
            vm((kc, 2, units // 2), BF), vm(ut.shape, BF), vm(adown.shape, BF), vm((16, capacity, kt + 128), BF),
            vm((n_t, sub, 128), F32), vm((n_t, sub, 128), F32), vm((n_t, sub, 128), BF),
            vm((2, 8, 128), F32), vm((2, CHUNKS, 128, cw), BF), vm((CHUNKS, 16 * rows, cw), F32),
        ] + both + sems,
        compiler_params=pltpu.CompilerParams(
            collective_id=0, has_side_effects=True, vmem_limit_bytes=67043328
        ),
    )(requests, routed, base, ut, adown)
    live = row_index < counts[group]
    return jnp.where(live[:, None], hidden, jnp.zeros_like(hidden))


def solution(mesh):
    placed = (
        P("dp", None),
        P("dp", None, "tensor"),
        P("dp", "tensor", None),
        P("dp", None, None, "tensor"),
        P("dp"),
        P(),
        P(),
    )
    return jax.shard_map(
        body, mesh=mesh, in_specs=placed, out_specs=P("dp", "tensor"), check_vma=False
    )
```

```python
import functools

import jax
import jax.numpy as jnp
from jax import lax
from jax.experimental import pallas as pl
from jax.experimental.pallas import tpu as pltpu
from jax.sharding import PartitionSpec as P

MESH = pl.DeviceIdType.MESH
BF = jnp.bfloat16
F32 = jnp.float32
CHUNKS = 7
NA = 4
NB = 3


def remote(src, dst, send, recv, dp, tensor):
    return pltpu.make_async_remote_copy(
        src_ref=src, dst_ref=dst, send_sem=send, recv_sem=recv,
        device_id=(dp, tensor), device_id_type=MESH,
    )


def kernel(
    x, wanted, positions, wt, ut, ad, out,
    piece, routed, wide, xe, we, wr, ur, av, arr, dpart, rsr, dfull, rx, dl, part,
    a2s, a2r, a1s, a1r, ays, ayr, bys, byr, b2s, b2r, b1s, b1r, hs, hid,
    loc, ro_s, ro_r, x_s, x_r, xl_s, xl_r, w_s, w_r, t1_s, t1_r, t2_s, t2_r, rx_s, rx_r, dl_s, dl_r,
    a2_s, a2_q, a1_s, a1_q, ay_s, ay_q, by_s, by_q, b2_s, b2_q, b1_s, b1_q, h_s, h_q,
):
    d = lax.axis_index("dp")
    t = lax.axis_index("tensor")
    n_t = lax.axis_size("tensor")
    chip, c = lax.div(d, 2), lax.rem(d, 2)
    z, y = lax.div(chip, 2), lax.rem(chip, 2)
    yo = 1 - y
    mate = chip * 2 + 1 - c
    zp, zm, z2 = lax.rem(z + 1, 4), lax.rem(z + 3, 4), lax.rem(z + 2, 4)
    to_zp = (zp * 2 + y) * 2 + c
    to_zm = (zm * 2 + y) * 2 + c
    to_y = (z * 2 + yo) * 2 + c
    kc = xe.shape[1] - 256
    kh = kc // 2
    cw = we.shape[2]
    hw = cw // 2
    sub = rsr.shape[1]

    half = hw * CHUNKS

    def units(h):
        return pl.ds(pl.multiple_of(h * half, 128), half)

    w_rows = wr.at[pl.ds(c * kh, kh)]
    own_w = pltpu.make_async_copy(wt.at[:, :, units(c)], w_rows, loc.at[0])
    own_u = pltpu.make_async_copy(ut, ur, loc.at[1])
    own_a = pltpu.make_async_copy(ad, av, loc.at[2])
    own_r = pltpu.make_async_copy(routed.at[d], arr.at[d], loc.at[3])
    x_mine = x.at[:, pl.ds(pl.multiple_of(chip * kc, 128), kc)]
    x_rows = xe.at[pl.ds(d * 64, 64), pl.ds(0, kc)]
    own_x = pltpu.make_async_copy(x_mine, x_rows, loc.at[4])
    own_p = pltpu.make_async_copy(
        x.at[:, pl.ds(pl.multiple_of(t * av.shape[1], 128), av.shape[1])], piece, loc.at[5]
    )
    own_p.start()
    own_a.start()
    own_x.start()
    own_w.start()
    own_u.start()

    barrier = pltpu.get_barrier_semaphore()

    @pl.loop(1, 16)
    def _(i):
        pl.semaphore_signal(barrier, inc=1, device_id=(lax.rem(d + i, 16), t), device_id_type=MESH)

    @pl.loop(1, n_t)
    def _(i):
        pl.semaphore_signal(barrier, inc=1, device_id=(d, lax.rem(t + i, n_t)), device_id_type=MESH)

    rows, kt = piece.shape
    named = (lax.broadcasted_iota(jnp.int32, (128, rows), 0) == wanted[...]).astype(F32).astype(BF)
    store = jnp.broadcast_to(positions[...].astype(F32), (8, 128)).astype(BF)
    slot = jnp.dot(store, named, preferred_element_type=F32)[0:1, :].astype(jnp.int32)
    owner, local = lax.div(slot, 8), lax.rem(slot, 8)
    owned = (lax.broadcasted_iota(jnp.int32, (16, rows), 0) == owner).astype(F32)
    upto = (
        lax.broadcasted_iota(jnp.int32, (rows, rows), 0) <= lax.broadcasted_iota(jnp.int32, (rows, rows), 1)
    ).astype(F32).astype(BF)
    seen = jnp.dot(owned.astype(BF), upto, preferred_element_type=F32)
    place = jnp.sum(owned * (seen - 1.0), axis=0, keepdims=True).astype(jnp.int32)
    select = (
        lax.broadcasted_iota(jnp.int32, (128, rows), 0) == owner * 8 + place
    ).astype(F32).astype(BF)
    kind = lax.broadcasted_iota(jnp.int32, (128, rows), 0)
    index = lax.broadcasted_iota(jnp.int32, (128, rows), 1)
    labels = jnp.where(kind == 0, local, jnp.where(kind == 1, index, 0)).astype(F32).astype(BF)
    routed[:, :, kt : kt + 128] = lax.dot_general(
        select, labels, (((1,), (1,)), ((), ())), preferred_element_type=F32
    ).reshape(16, 8, 128).astype(BF)
    own_p.wait()
    routed[:, :, 0:kt] = jnp.dot(
        select, piece[...], preferred_element_type=F32
    ).reshape(16, 8, kt).astype(BF)
    own_r.start()

    pl.semaphore_wait(barrier, 15 + n_t - 1)

    def routed_copy(i):
        peer = lax.rem(d + i, 16)
        return remote(routed.at[peer], arr.at[d], ro_s.at[i], ro_r.at[i], peer, t)

    def x_copy(i):
        q = lax.rem(chip + i, 8)
        src = x.at[:, pl.ds(pl.multiple_of(q * kc, 128), kc)]
        return remote(src, x_rows, x_s.at[i], x_r.at[i], q * 2 + c, t)

    def x_relay(i):
        block = (lax.rem(chip + 8 - i, 8)) * 2 + c
        rows = xe.at[pl.ds(block * 64, 64), pl.ds(0, kc)]
        return remote(rows, rows, xl_s.at[i], xl_r.at[i], mate, t)

    @pl.loop(1, 16)
    def _(i):
        routed_copy(i).start()

    @pl.loop(1, 8)
    def _(i):
        x_copy(i).start()

    x_own_mate = remote(x_mine, x_rows, xl_s.at[0], xl_r.at[0], mate, t)
    x_own_mate.start()
    w_mate = remote(wt.at[:, :, units(1 - c)], w_rows, w_s, w_r, mate, t)
    w_mate.start()

    to = lax.broadcasted_iota(jnp.int32, (256, 256), 0)
    at = lax.broadcasted_iota(jnp.int32, (256, 256), 1)
    parting = (at == lax.rem(to, 128) * 2 + lax.div(to, 128)).astype(F32).astype(BF)
    blocks = kh // 128

    def part_weight(owner):
        @pl.loop(0, blocks)
        def _(i):
            b = owner * blocks + i
            rows = pl.ds(pl.multiple_of(b * 128, 128), 128)
            for j in range(CHUNKS):
                pairs = wr[rows, :, j * hw : j * hw + hw].reshape(256, hw)
                parted = jnp.dot(parting, pairs, preferred_element_type=F32).astype(BF)
                we[j, rows, 0:hw] = parted[0:128]
                we[j, rows, hw:cw] = parted[128:256]

    own_w.wait()
    part_weight(c)

    own_r.wait()
    own_a.wait()

    @pl.loop(1, 16)
    def _(i):
        routed_copy(i).wait_recv()

    rows_in = arr[...].astype(F32).reshape(128, kt + 128)
    body_in = rows_in[:, :kt].astype(BF)
    lab = rows_in[:, kt:]
    which = lab[:, 0:1].astype(jnp.int32)
    down = jnp.zeros((128, 128), F32)
    for a in range(8):
        term = jnp.dot(body_in, av[a], preferred_element_type=F32)
        down = down + jnp.where(which == a, term, 0.0)
    dpart[...] = down.reshape(n_t, sub, 128)

    def t1_copy(i):
        peer = lax.rem(t + i, n_t)
        return remote(dpart.at[peer], rsr.at[i], t1_s.at[i], t1_r.at[i], d, peer)

    def t2_copy(i):
        peer = lax.rem(t + i, n_t)
        return remote(dfull.at[t], dfull.at[t], t2_s.at[i], t2_r.at[i], d, peer)

    @pl.loop(1, n_t)
    def _(i):
        t1_copy(i).start()

    pick = (lax.broadcasted_iota(jnp.int32, (8, 128), 1) == 1).astype(BF)
    rx[c] = lax.dot_general(
        pick, lab.astype(BF), (((1,), (1,)), ((), ())), preferred_element_type=F32
    )
    rx_copy = remote(rx.at[c], rx.at[c], rx_s, rx_r, mate, t)
    rx_copy.start()

    total = dpart[t]

    @pl.loop(1, n_t)
    def _(i):
        t1_copy(i).wait_recv()

    for i in range(1, n_t):
        total = total + rsr[i]
    dfull[t] = total.astype(BF)

    @pl.loop(1, n_t)
    def _(i):
        t2_copy(i).start()

    @pl.loop(1, 8)
    def _(i):
        x_copy(i).wait_recv()
        x_relay(i).start()

    w_mate.wait_recv()
    part_weight(1 - c)
    rx_copy.wait_recv()
    for core in range(2):
        target = lax.broadcasted_iota(jnp.int32, (1024, 128), 1) // 8 * 64 + rx[core][0:1, :].astype(jnp.int32)
        hot = lax.broadcasted_iota(jnp.int32, (1024, 128), 0) == target
        xe[:, kc + core * 128 : kc + core * 128 + 128] = hot.astype(F32).astype(BF)

    @pl.loop(1, n_t)
    def _(i):
        t2_copy(i).wait_recv()

    downs = dfull[...].astype(F32).reshape(128, 128).astype(BF)
    deep = 2 * ur.shape[0]
    lane = lax.broadcasted_iota(jnp.int32, (128, deep), 1)
    src = lax.broadcasted_iota(jnp.int32, (128, deep), 0)
    mine = lax.div(lane, 128) == which
    rank = lax.div(lax.rem(lane, 128), 2)

    def spread(which_term):
        pattern = (src == rank + 64 * which_term).astype(F32).astype(BF)
        copies = jnp.dot(downs, pattern, preferred_element_type=F32)
        return jnp.where(mine & (lax.rem(lane, 2) == which_term), copies, 0.0).astype(BF)

    wide[0:128] = spread(0)
    wide[128:256] = spread(1)
    own_u.wait()

    def dl_copy(j):
        return remote(
            dl.at[1 - c, j], we.at[j, pl.ds(kc + c * 128, 128), :], dl_s.at[j], dl_r.at[j], mate, t
        )

    def adapter_terms(j):
        for h in range(2):
            cols = pl.ds(pl.multiple_of(h * half + j * hw, 128), hw)
            both = jnp.dot(
                wide[...], ur[:, :, cols].reshape(deep, hw), preferred_element_type=F32
            ).astype(BF)
            dl[h, j, :, 0:hw] = both[0:128]
            dl[h, j, :, hw:cw] = both[128:256]
        dl_copy(j).start()
        we[j, pl.ds(pl.multiple_of(kc + c * 128, 128), 128), :] = dl[c, j]

    @pl.loop(0, 2)
    def _(j):
        adapter_terms(j)

    own_x.wait()
    x_own_mate.wait_recv()

    @pl.loop(1, 8)
    def _(i):
        x_relay(i).wait_recv()

    def compute(k, first, count):
        @pl.loop(0, count)
        def _(i):
            zz = lax.rem(z + first + i, 4)
            rows = pl.ds(pl.multiple_of(zz * 256, 256), 256)
            part[k, rows, :] = jnp.dot(xe[rows, :], we[k], preferred_element_type=F32)

    def rows_of(zz, yy):
        return pl.ds(pl.multiple_of(zz * 256 + yy * 128, 128), 128)

    def half_of(zz, yy, cc):
        return pl.ds(pl.multiple_of(zz * 256 + yy * 128 + cc * 64, 64), 64)

    def ra2(s, w):
        return remote(a2s.at[s, w], a2r.at[s, w], a2_s.at[s, w], a2_q.at[s, w], (to_zp, to_zm)[w], t)

    def ra1(s, w, p):
        return remote(a1s.at[s, w, p], a1r.at[s, w, p], a1_s.at[s, w, p], a1_q.at[s, w, p], (to_zp, to_zm)[w], t)

    def ray(s):
        return remote(ays.at[s], ayr.at[s], ay_s.at[s], ay_q.at[s], to_y, t)

    def rby(s, i):
        return remote(bys.at[s, i], byr.at[s, i], by_s.at[s, i], by_q.at[s, i], to_y, t)

    def rb2(s, w):
        return remote(b2s.at[s, w], b2r.at[s, w], b2_s.at[s, w], b2_q.at[s, w], (to_zp, to_zm)[w], t)

    def rb1(s, w, p):
        return remote(b1s.at[s, w, p], b1r.at[s, w, p], b1_s.at[s, w, p], b1_q.at[s, w, p], (to_zp, to_zm)[w], t)

    def rh(k):
        return remote(
            hs.at[k, 1 - c], hid.at[c, :, pl.ds(pl.multiple_of(k * hw, 128), hw)],
            h_s.at[k], h_q.at[k], mate, t,
        )

    def a_first(s):
        k = 2 * s
        dl_copy(k).wait_recv()
        compute(k, 1, 3)
        a2s[s, 0] = part[k, rows_of(z2, 0), :].astype(BF)
        ra2(s, 0).start()
        a2s[s, 1] = part[k, rows_of(z2, 1), :].astype(BF)
        ra2(s, 1).start()
        a1s[s, 0, 1] = part[k, rows_of(zp, 1), :].astype(BF)
        ra1(s, 0, 1).start()
        a1s[s, 1, 1] = part[k, rows_of(zm, 0), :].astype(BF)
        ra1(s, 1, 1).start()

    def a_pass(s):
        k = 2 * s
        for w, zz in ((0, zp), (1, zm)):
            ra2(s, w).wait_recv()
            a1s[s, w, 0] = (part[k, rows_of(zz, w), :] + a2r[s, w].astype(F32)).astype(BF)
            ra1(s, w, 0).start()

    def a_cross(s):
        k = 2 * s
        compute(k, 0, 1)
        for w in range(2):
            for p in range(2):
                ra1(s, w, p).wait_recv()
        ays[s] = (
            part[k, rows_of(z, yo), :] + a1r[s, yo, 0].astype(F32) + a1r[s, y, 1].astype(F32)
        ).astype(BF)
        ray(s).start()
        part[k, rows_of(z, y), :] = (
            part[k, rows_of(z, y), :] + a1r[s, y, 0].astype(F32) + a1r[s, yo, 1].astype(F32)
        )

    def finish(k, cc, total):
        gate, up = total[:, :hw], total[:, hw:]
        hs[k, cc] = (gate / (1.0 + jnp.exp(-gate)) * up).astype(BF)

    def deliver(k):
        rh(k).start()
        hid[c, :, pl.ds(pl.multiple_of(k * hw, 128), hw)] = hs[k, c]

    def a_last(s):
        k = 2 * s
        ray(s).wait_recv()
        for cc in range(2):
            finish(k, cc, part[k, half_of(z, y, cc), :] + ayr[s, cc * 64 : cc * 64 + 64, :].astype(F32))
        deliver(k)

    def b_first(s):
        k = 2 * s + 1
        dl_copy(k).wait_recv()
        compute(k, 0, 4)
        for i in (2, 1, 3, 0):
            zz = lax.rem(z + i, 4)
            bys[s, i] = part[k, rows_of(zz, yo), :].astype(BF)
            rby(s, i).start()

    def b_second(s):
        k = 2 * s + 1
        rby(s, 2).wait_recv()
        for cc in range(2):
            b2s[s, cc] = (
                part[k, half_of(z2, y, cc), :] + byr[s, 2, cc * 64 : cc * 64 + 64, :].astype(F32)
            ).astype(BF)
            rb2(s, cc).start()
        for w, zz, i in ((0, zp, 1), (1, zm, 3)):
            rby(s, i).wait_recv()
            o = 1 - w
            b1s[s, w, 1] = (
                part[k, half_of(zz, y, o), :] + byr[s, i, o * 64 : o * 64 + 64, :].astype(F32)
            ).astype(BF)
            rb1(s, w, 1).start()

    def b_pass(s):
        k = 2 * s + 1
        for w, zz, i in ((0, zp, 1), (1, zm, 3)):
            rb2(s, w).wait_recv()
            b1s[s, w, 0] = (
                part[k, half_of(zz, y, w), :]
                + byr[s, i, w * 64 : w * 64 + 64, :].astype(F32)
                + b2r[s, w].astype(F32)
            ).astype(BF)
            rb1(s, w, 0).start()

    def b_last(s):
        k = 2 * s + 1
        rby(s, 0).wait_recv()
        for w in range(2):
            for p in range(2):
                rb1(s, w, p).wait_recv()
        for cc in range(2):
            finish(
                k, cc,
                part[k, half_of(z, y, cc), :]
                + byr[s, 0, cc * 64 : cc * 64 + 64, :].astype(F32)
                + b1r[s, cc, 0].astype(F32)
                + b1r[s, 1 - cc, 1].astype(F32),
            )
        deliver(k)

    @pl.loop(0, NA)
    def _(s):
        a_first(s)

        @pl.when(s < NB)
        def _():
            adapter_terms(2 * s + 2)
            b_first(s)

        @pl.when(s < NB - 1)
        def _():
            adapter_terms(2 * s + 3)

    @pl.loop(0, NA)
    def _(s):
        a_pass(s)

    @pl.loop(0, NA)
    def _(s):
        a_cross(s)

        @pl.when(s < NB)
        def _():
            b_second(s)

    @pl.loop(0, NB)
    def _(s):
        b_pass(s)

    @pl.loop(0, NA)
    def _(s):
        a_last(s)

    @pl.loop(0, NB)
    def _(s):
        b_last(s)

    @pl.loop(0, CHUNKS)
    def _(k):
        rh(k).wait_recv()

    out[:, 0:half] = hid[0]
    out[:, half : 2 * half] = hid[1]

    @pl.loop(1, 16)
    def _(i):
        routed_copy(i).wait_send()

    @pl.loop(1, 8)
    def _(i):
        x_copy(i).wait_send()
        x_relay(i).wait_send()

    x_own_mate.wait_send()
    w_mate.wait_send()
    rx_copy.wait_send()

    @pl.loop(1, n_t)
    def _(i):
        t1_copy(i).wait_send()
        t2_copy(i).wait_send()

    @pl.loop(0, NA)
    def _(s):
        ray(s).wait_send()
        for w in range(2):
            ra2(s, w).wait_send()
            for p in range(2):
                ra1(s, w, p).wait_send()

    @pl.loop(0, NB)
    def _(s):
        for i in range(4):
            rby(s, i).wait_send()
        for w in range(2):
            rb2(s, w).wait_send()
            for p in range(2):
                rb1(s, w, p).wait_send()

    @pl.loop(0, CHUNKS)
    def _(k):
        rh(k).wait_send()
        dl_copy(k).wait_send()


def body(requests, base, adown, aup, request_adapter, adapter_position, counts):
    rows, width = requests.shape
    n_t = lax.axis_size("tensor")
    group = lax.axis_index("dp")
    units = base.shape[2]
    per_owner, kt, rank2 = adown.shape
    capacity = 8
    row_index = jnp.arange(rows, dtype=jnp.int32)

    ut = aup.reshape(aup.shape[0] * aup.shape[1], 2, units)
    kc = width // 8
    hw = units // (2 * CHUNKS)
    cw = 2 * hw
    sub = 128 // n_t
    vm, dma = pltpu.VMEM, pltpu.SemaphoreType.DMA
    both = [
        vm((NA, 2, 128, cw), BF), vm((NA, 2, 128, cw), BF),
        vm((NA, 2, 2, 128, cw), BF), vm((NA, 2, 2, 128, cw), BF),
        vm((NA, 128, cw), BF), vm((NA, 128, cw), BF),
        vm((NB, 4, 128, cw), BF), vm((NB, 4, 128, cw), BF),
        vm((NB, 2, 64, cw), BF), vm((NB, 2, 64, cw), BF),
        vm((NB, 2, 2, 64, cw), BF), vm((NB, 2, 2, 64, cw), BF),
        vm((CHUNKS, 2, 64, hw), BF), vm((2, 64, hw * CHUNKS), BF),
    ]
    sems = [
        dma((6,)), dma((16,)), dma((16,)), dma((8,)), dma((8,)), dma((8,)), dma((8,)),
        dma, dma, dma((n_t,)), dma((n_t,)), dma((n_t,)), dma((n_t,)), dma, dma, dma((CHUNKS,)), dma((CHUNKS,)),
        dma((NA, 2)), dma((NA, 2)), dma((NA, 2, 2)), dma((NA, 2, 2)), dma((NA,)), dma((NA,)),
        dma((NB, 4)), dma((NB, 4)), dma((NB, 2)), dma((NB, 2)), dma((NB, 2, 2)), dma((NB, 2, 2)),
        dma((CHUNKS,)), dma((CHUNKS,)),
    ]
    hidden = pl.pallas_call(
        kernel,
        out_shape=jax.ShapeDtypeStruct((rows, units), BF),
        in_specs=[pl.BlockSpec(memory_space=pl.ANY)]
        + [pl.BlockSpec(memory_space=pltpu.VMEM)] * 2
        + [pl.BlockSpec(memory_space=pl.ANY)] * 3,
        out_specs=pl.BlockSpec(memory_space=pltpu.VMEM),
        scratch_shapes=[
            vm((rows, kt), BF), vm((16, capacity, kt + 128), BF), vm((256, 2 * ut.shape[0]), BF),
            vm((16 * rows, kc + 256), BF), vm((CHUNKS, kc + 256, cw), BF),
            vm((kc, 2, units // 2), BF), vm(ut.shape, BF), vm(adown.shape, BF), vm((16, capacity, kt + 128), BF),
            vm((n_t, sub, 128), F32), vm((n_t, sub, 128), F32), vm((n_t, sub, 128), BF),
            vm((2, 8, 128), F32), vm((2, CHUNKS, 128, cw), BF), vm((CHUNKS, 16 * rows, cw), F32),
        ] + both + sems,
        compiler_params=pltpu.CompilerParams(
            collective_id=0, has_side_effects=True, vmem_limit_bytes=67043328
        ),
    )(requests, request_adapter.reshape(1, rows), adapter_position.reshape(1, -1), base, ut, adown)
    live = row_index < counts[group]
    return jnp.where(live[:, None], hidden, jnp.zeros_like(hidden))


def solution(mesh):
    placed = (
        P("dp", None),
        P("dp", None, "tensor"),
        P("dp", "tensor", None),
        P("dp", None, None, "tensor"),
        P("dp"),
        P(),
        P(),
    )
    return jax.shard_map(
        body, mesh=mesh, in_specs=placed, out_specs=P("dp", "tensor"), check_vma=False
    )
```

```python
import functools

import jax
import jax.numpy as jnp
from jax import lax
from jax.experimental import pallas as pl
from jax.experimental.pallas import tpu as pltpu
from jax.sharding import PartitionSpec as P

MESH = pl.DeviceIdType.MESH
BF = jnp.bfloat16
F32 = jnp.float32
CHUNKS = 7
NA = 4
NB = 3


def remote(src, dst, send, recv, dp, tensor):
    return pltpu.make_async_remote_copy(
        src_ref=src, dst_ref=dst, send_sem=send, recv_sem=recv,
        device_id=(dp, tensor), device_id_type=MESH,
    )


def kernel(
    x, wanted, positions, wt, ut, ad, out,
    piece, routed, wide, xe, we, wr, ur, av, arr, dpart, rsr, dfull, rx, dl, part,
    a2s, a2r, a1s, a1r, ays, ayr, bys, byr, b2s, b2r, b1s, b1r, hs, hid,
    loc, ro_s, ro_r, x_s, x_r, xl_s, xl_r, w_s, w_r, t1_s, t1_r, t2_s, t2_r, rx_s, rx_r, dl_s, dl_r,
    a2_s, a2_q, a1_s, a1_q, ay_s, ay_q, by_s, by_q, b2_s, b2_q, b1_s, b1_q, h_s, h_q,
):
    d = lax.axis_index("dp")
    t = lax.axis_index("tensor")
    n_t = lax.axis_size("tensor")
    chip, c = lax.div(d, 2), lax.rem(d, 2)
    z, y = lax.div(chip, 2), lax.rem(chip, 2)
    yo = 1 - y
    mate = chip * 2 + 1 - c
    zp, zm, z2 = lax.rem(z + 1, 4), lax.rem(z + 3, 4), lax.rem(z + 2, 4)
    to_zp = (zp * 2 + y) * 2 + c
    to_zm = (zm * 2 + y) * 2 + c
    to_y = (z * 2 + yo) * 2 + c
    kc = xe.shape[1] - 256
    kh = kc // 2
    cw = we.shape[2]
    hw = cw // 2
    sub = rsr.shape[1]

    half = hw * CHUNKS

    def units(h):
        return pl.ds(pl.multiple_of(h * half, 128), half)

    w_rows = wr.at[pl.ds(c * kh, kh)]
    own_w = pltpu.make_async_copy(wt.at[:, :, units(c)], w_rows, loc.at[0])
    own_u = pltpu.make_async_copy(ut, ur, loc.at[1])
    own_a = pltpu.make_async_copy(ad, av, loc.at[2])
    own_r = pltpu.make_async_copy(routed.at[d], arr.at[d], loc.at[3])
    x_mine = x.at[:, pl.ds(pl.multiple_of(chip * kc, 128), kc)]
    x_rows = xe.at[pl.ds(d * 64, 64), pl.ds(0, kc)]
    own_x = pltpu.make_async_copy(x_mine, x_rows, loc.at[4])
    own_p = pltpu.make_async_copy(
        x.at[:, pl.ds(pl.multiple_of(t * av.shape[1], 128), av.shape[1])], piece, loc.at[5]
    )
    own_p.start()
    own_a.start()
    own_x.start()
    own_w.start()
    own_u.start()

    barrier = pltpu.get_barrier_semaphore()

    @pl.loop(1, 16)
    def _(i):
        pl.semaphore_signal(barrier, inc=1, device_id=(lax.rem(d + i, 16), t), device_id_type=MESH)

    @pl.loop(1, n_t)
    def _(i):
        pl.semaphore_signal(barrier, inc=1, device_id=(d, lax.rem(t + i, n_t)), device_id_type=MESH)

    rows, kt = piece.shape
    named = (lax.broadcasted_iota(jnp.int32, (128, rows), 0) == wanted[...]).astype(F32).astype(BF)
    store = jnp.broadcast_to(positions[...].astype(F32), (8, 128)).astype(BF)
    slot = jnp.dot(store, named, preferred_element_type=F32)[0:1, :].astype(jnp.int32)
    owner, local = lax.div(slot, 8), lax.rem(slot, 8)
    owned = (lax.broadcasted_iota(jnp.int32, (16, rows), 0) == owner).astype(F32)
    upto = (
        lax.broadcasted_iota(jnp.int32, (rows, rows), 0) <= lax.broadcasted_iota(jnp.int32, (rows, rows), 1)
    ).astype(F32).astype(BF)
    seen = jnp.dot(owned.astype(BF), upto, preferred_element_type=F32)
    place = jnp.sum(owned * (seen - 1.0), axis=0, keepdims=True).astype(jnp.int32)
    select = (
        lax.broadcasted_iota(jnp.int32, (128, rows), 0) == owner * 8 + place
    ).astype(F32).astype(BF)
    kind = lax.broadcasted_iota(jnp.int32, (128, rows), 0)
    index = lax.broadcasted_iota(jnp.int32, (128, rows), 1)
    labels = jnp.where(kind == 0, local, jnp.where(kind == 1, index, 0)).astype(F32).astype(BF)
    routed[:, :, kt : kt + 128] = lax.dot_general(
        select, labels, (((1,), (1,)), ((), ())), preferred_element_type=F32
    ).reshape(16, 8, 128).astype(BF)
    own_p.wait()
    routed[:, :, 0:kt] = jnp.dot(
        select, piece[...], preferred_element_type=F32
    ).reshape(16, 8, kt).astype(BF)
    own_r.start()

    pl.semaphore_wait(barrier, 15 + n_t - 1)

    def routed_copy(i):
        peer = lax.rem(d + i, 16)
        return remote(routed.at[peer], arr.at[d], ro_s.at[i], ro_r.at[i], peer, t)

    def x_copy(i):
        q = lax.rem(chip + i, 8)
        src = x.at[:, pl.ds(pl.multiple_of(q * kc, 128), kc)]
        return remote(src, x_rows, x_s.at[i], x_r.at[i], q * 2 + c, t)

    def x_relay(i):
        block = (lax.rem(chip + 8 - i, 8)) * 2 + c
        rows = xe.at[pl.ds(block * 64, 64), pl.ds(0, kc)]
        return remote(rows, rows, xl_s.at[i], xl_r.at[i], mate, t)

    @pl.loop(1, 16)
    def _(i):
        routed_copy(i).start()

    @pl.loop(1, 8)
    def _(i):
        x_copy(i).start()

    x_own_mate = remote(x_mine, x_rows, xl_s.at[0], xl_r.at[0], mate, t)
    x_own_mate.start()

    def w_copy(j):
        src = wt.at[:, :, pl.ds(pl.multiple_of((1 - c) * half + j * hw, 128), hw)]
        dst = wr.at[pl.ds(c * kh, kh), :, pl.ds(pl.multiple_of(j * hw, 128), hw)]
        return remote(src, dst, w_s.at[j], w_r.at[j], mate, t)

    @pl.loop(0, CHUNKS)
    def _(j):
        w_copy(j).start()

    to = lax.broadcasted_iota(jnp.int32, (256, 256), 0)
    at = lax.broadcasted_iota(jnp.int32, (256, 256), 1)
    parting = (at == lax.rem(to, 128) * 2 + lax.div(to, 128)).astype(F32).astype(BF)
    blocks = kh // 128

    def part_weight(core, j):
        @pl.loop(0, blocks)
        def _(i):
            rows = pl.ds(pl.multiple_of((core * blocks + i) * 128, 128), 128)
            pairs = wr[rows, :, pl.ds(pl.multiple_of(j * hw, 128), hw)].reshape(256, hw)
            parted = jnp.dot(parting, pairs, preferred_element_type=F32).astype(BF)
            we[j, rows, 0:hw] = parted[0:128]
            we[j, rows, hw:cw] = parted[128:256]

    own_w.wait()

    @pl.loop(0, 2)
    def _(j):
        part_weight(c, j)

    own_r.wait()
    own_a.wait()

    @pl.loop(1, 16)
    def _(i):
        routed_copy(i).wait_recv()

    rows_in = arr[...].astype(F32).reshape(128, kt + 128)
    body_in = rows_in[:, :kt].astype(BF)
    lab = rows_in[:, kt:]
    which = lab[:, 0:1].astype(jnp.int32)
    down = jnp.zeros((128, 128), F32)
    for a in range(8):
        term = jnp.dot(body_in, av[a], preferred_element_type=F32)
        down = down + jnp.where(which == a, term, 0.0)
    dpart[...] = down.reshape(n_t, sub, 128)

    def t1_copy(i):
        peer = lax.rem(t + i, n_t)
        return remote(dpart.at[peer], rsr.at[i], t1_s.at[i], t1_r.at[i], d, peer)

    def t2_copy(i):
        peer = lax.rem(t + i, n_t)
        return remote(dfull.at[t], dfull.at[t], t2_s.at[i], t2_r.at[i], d, peer)

    @pl.loop(1, n_t)
    def _(i):
        t1_copy(i).start()

    pick = (lax.broadcasted_iota(jnp.int32, (8, 128), 1) == 1).astype(BF)
    rx[c] = lax.dot_general(
        pick, lab.astype(BF), (((1,), (1,)), ((), ())), preferred_element_type=F32
    )
    rx_copy = remote(rx.at[c], rx.at[c], rx_s, rx_r, mate, t)
    rx_copy.start()

    total = dpart[t]

    @pl.loop(1, n_t)
    def _(i):
        t1_copy(i).wait_recv()

    for i in range(1, n_t):
        total = total + rsr[i]
    dfull[t] = total.astype(BF)

    @pl.loop(1, n_t)
    def _(i):
        t2_copy(i).start()

    @pl.loop(1, 8)
    def _(i):
        x_copy(i).wait_recv()
        x_relay(i).start()

    @pl.loop(0, 2)
    def _(j):
        w_copy(j).wait_recv()
        part_weight(1 - c, j)

    rx_copy.wait_recv()
    for core in range(2):
        target = lax.broadcasted_iota(jnp.int32, (1024, 128), 1) // 8 * 64 + rx[core][0:1, :].astype(jnp.int32)
        hot = lax.broadcasted_iota(jnp.int32, (1024, 128), 0) == target
        xe[:, kc + core * 128 : kc + core * 128 + 128] = hot.astype(F32).astype(BF)

    @pl.loop(1, n_t)
    def _(i):
        t2_copy(i).wait_recv()

    downs = dfull[...].astype(F32).reshape(128, 128).astype(BF)
    deep = 2 * ur.shape[0]
    lane = lax.broadcasted_iota(jnp.int32, (128, deep), 1)
    src = lax.broadcasted_iota(jnp.int32, (128, deep), 0)
    mine = lax.div(lane, 128) == which
    rank = lax.div(lax.rem(lane, 128), 2)

    def spread(which_term):
        pattern = (src == rank + 64 * which_term).astype(F32).astype(BF)
        copies = jnp.dot(downs, pattern, preferred_element_type=F32)
        return jnp.where(mine & (lax.rem(lane, 2) == which_term), copies, 0.0).astype(BF)

    wide[0:128] = spread(0)
    wide[128:256] = spread(1)
    own_u.wait()

    def dl_copy(j):
        return remote(
            dl.at[1 - c, j], we.at[j, pl.ds(kc + c * 128, 128), :], dl_s.at[j], dl_r.at[j], mate, t
        )

    def adapter_terms(j):
        for h in range(2):
            cols = pl.ds(pl.multiple_of(h * half + j * hw, 128), hw)
            both = jnp.dot(
                wide[...], ur[:, :, cols].reshape(deep, hw), preferred_element_type=F32
            ).astype(BF)
            dl[h, j, :, 0:hw] = both[0:128]
            dl[h, j, :, hw:cw] = both[128:256]
        dl_copy(j).start()
        we[j, pl.ds(pl.multiple_of(kc + c * 128, 128), 128), :] = dl[c, j]

    def prepare(j):
        adapter_terms(j)
        part_weight(c, j)
        w_copy(j).wait_recv()
        part_weight(1 - c, j)

    @pl.loop(0, 2)
    def _(j):
        adapter_terms(j)

    own_x.wait()
    x_own_mate.wait_recv()

    @pl.loop(1, 8)
    def _(i):
        x_relay(i).wait_recv()

    def compute(k, first, count):
        @pl.loop(0, count)
        def _(i):
            zz = lax.rem(z + first + i, 4)
            rows = pl.ds(pl.multiple_of(zz * 256, 256), 256)
            part[k, rows, :] = jnp.dot(xe[rows, :], we[k], preferred_element_type=F32)

    def rows_of(zz, yy):
        return pl.ds(pl.multiple_of(zz * 256 + yy * 128, 128), 128)

    def half_of(zz, yy, cc):
        return pl.ds(pl.multiple_of(zz * 256 + yy * 128 + cc * 64, 64), 64)

    def ra2(s, w):
        return remote(a2s.at[s, w], a2r.at[s, w], a2_s.at[s, w], a2_q.at[s, w], (to_zp, to_zm)[w], t)

    def ra1(s, w, p):
        return remote(a1s.at[s, w, p], a1r.at[s, w, p], a1_s.at[s, w, p], a1_q.at[s, w, p], (to_zp, to_zm)[w], t)

    def ray(s):
        return remote(ays.at[s], ayr.at[s], ay_s.at[s], ay_q.at[s], to_y, t)

    def rby(s, i):
        return remote(bys.at[s, i], byr.at[s, i], by_s.at[s, i], by_q.at[s, i], to_y, t)

    def rb2(s, w):
        return remote(b2s.at[s, w], b2r.at[s, w], b2_s.at[s, w], b2_q.at[s, w], (to_zp, to_zm)[w], t)

    def rb1(s, w, p):
        return remote(b1s.at[s, w, p], b1r.at[s, w, p], b1_s.at[s, w, p], b1_q.at[s, w, p], (to_zp, to_zm)[w], t)

    def rh(k):
        return remote(
            hs.at[k, 1 - c], hid.at[c, :, pl.ds(pl.multiple_of(k * hw, 128), hw)],
            h_s.at[k], h_q.at[k], mate, t,
        )

    def a_first(s):
        k = 2 * s
        dl_copy(k).wait_recv()
        compute(k, 1, 3)
        a2s[s, 0] = part[k, rows_of(z2, 0), :].astype(BF)
        ra2(s, 0).start()
        a2s[s, 1] = part[k, rows_of(z2, 1), :].astype(BF)
        ra2(s, 1).start()
        a1s[s, 0, 1] = part[k, rows_of(zp, 1), :].astype(BF)
        ra1(s, 0, 1).start()
        a1s[s, 1, 1] = part[k, rows_of(zm, 0), :].astype(BF)
        ra1(s, 1, 1).start()

    def a_pass(s):
        k = 2 * s
        for w, zz in ((0, zp), (1, zm)):
            ra2(s, w).wait_recv()
            a1s[s, w, 0] = (part[k, rows_of(zz, w), :] + a2r[s, w].astype(F32)).astype(BF)
            ra1(s, w, 0).start()

    def a_cross(s):
        k = 2 * s
        compute(k, 0, 1)
        for w in range(2):
            for p in range(2):
                ra1(s, w, p).wait_recv()
        ays[s] = (
            part[k, rows_of(z, yo), :] + a1r[s, yo, 0].astype(F32) + a1r[s, y, 1].astype(F32)
        ).astype(BF)
        ray(s).start()
        part[k, rows_of(z, y), :] = (
            part[k, rows_of(z, y), :] + a1r[s, y, 0].astype(F32) + a1r[s, yo, 1].astype(F32)
        )

    def finish(k, cc, total):
        gate, up = total[:, :hw], total[:, hw:]
        hs[k, cc] = (gate / (1.0 + jnp.exp(-gate)) * up).astype(BF)

    def deliver(k):
        rh(k).start()
        hid[c, :, pl.ds(pl.multiple_of(k * hw, 128), hw)] = hs[k, c]

    def a_last(s):
        k = 2 * s
        ray(s).wait_recv()
        for cc in range(2):
            finish(k, cc, part[k, half_of(z, y, cc), :] + ayr[s, cc * 64 : cc * 64 + 64, :].astype(F32))
        deliver(k)

    def b_first(s):
        k = 2 * s + 1
        dl_copy(k).wait_recv()
        compute(k, 0, 4)
        for i in (2, 1, 3, 0):
            zz = lax.rem(z + i, 4)
            bys[s, i] = part[k, rows_of(zz, yo), :].astype(BF)
            rby(s, i).start()

    def b_second(s):
        k = 2 * s + 1
        rby(s, 2).wait_recv()
        for cc in range(2):
            b2s[s, cc] = (
                part[k, half_of(z2, y, cc), :] + byr[s, 2, cc * 64 : cc * 64 + 64, :].astype(F32)
            ).astype(BF)
            rb2(s, cc).start()
        for w, zz, i in ((0, zp, 1), (1, zm, 3)):
            rby(s, i).wait_recv()
            o = 1 - w
            b1s[s, w, 1] = (
                part[k, half_of(zz, y, o), :] + byr[s, i, o * 64 : o * 64 + 64, :].astype(F32)
            ).astype(BF)
            rb1(s, w, 1).start()

    def b_pass(s):
        k = 2 * s + 1
        for w, zz, i in ((0, zp, 1), (1, zm, 3)):
            rb2(s, w).wait_recv()
            b1s[s, w, 0] = (
                part[k, half_of(zz, y, w), :]
                + byr[s, i, w * 64 : w * 64 + 64, :].astype(F32)
                + b2r[s, w].astype(F32)
            ).astype(BF)
            rb1(s, w, 0).start()

    def b_last(s):
        k = 2 * s + 1
        rby(s, 0).wait_recv()
        for w in range(2):
            for p in range(2):
                rb1(s, w, p).wait_recv()
        for cc in range(2):
            finish(
                k, cc,
                part[k, half_of(z, y, cc), :]
                + byr[s, 0, cc * 64 : cc * 64 + 64, :].astype(F32)
                + b1r[s, cc, 0].astype(F32)
                + b1r[s, 1 - cc, 1].astype(F32),
            )
        deliver(k)

    @pl.loop(0, NA)
    def _(s):
        a_first(s)

        @pl.when(s < NB)
        def _():
            b_first(s)
            prepare(2 * s + 2)

        @pl.when(s < NB - 1)
        def _():
            prepare(2 * s + 3)

    @pl.loop(0, NA)
    def _(s):
        a_pass(s)

    @pl.loop(0, NA)
    def _(s):
        a_cross(s)

        @pl.when(s < NB)
        def _():
            b_second(s)

    @pl.loop(0, NB)
    def _(s):
        b_pass(s)

    @pl.loop(0, NA)
    def _(s):
        a_last(s)

    @pl.loop(0, NB)
    def _(s):
        b_last(s)

    @pl.loop(0, CHUNKS)
    def _(k):
        rh(k).wait_recv()

    out[:, 0:half] = hid[0]
    out[:, half : 2 * half] = hid[1]

    @pl.loop(1, 16)
    def _(i):
        routed_copy(i).wait_send()

    @pl.loop(1, 8)
    def _(i):
        x_copy(i).wait_send()
        x_relay(i).wait_send()

    x_own_mate.wait_send()
    rx_copy.wait_send()

    @pl.loop(1, n_t)
    def _(i):
        t1_copy(i).wait_send()
        t2_copy(i).wait_send()

    @pl.loop(0, NA)
    def _(s):
        ray(s).wait_send()
        for w in range(2):
            ra2(s, w).wait_send()
            for p in range(2):
                ra1(s, w, p).wait_send()

    @pl.loop(0, NB)
    def _(s):
        for i in range(4):
            rby(s, i).wait_send()
        for w in range(2):
            rb2(s, w).wait_send()
            for p in range(2):
                rb1(s, w, p).wait_send()

    @pl.loop(0, CHUNKS)
    def _(k):
        rh(k).wait_send()
        dl_copy(k).wait_send()
        w_copy(k).wait_send()


def body(requests, base, adown, aup, request_adapter, adapter_position, counts):
    rows, width = requests.shape
    n_t = lax.axis_size("tensor")
    group = lax.axis_index("dp")
    units = base.shape[2]
    per_owner, kt, rank2 = adown.shape
    capacity = 8
    row_index = jnp.arange(rows, dtype=jnp.int32)

    ut = aup.reshape(aup.shape[0] * aup.shape[1], 2, units)
    kc = width // 8
    hw = units // (2 * CHUNKS)
    cw = 2 * hw
    sub = 128 // n_t
    vm, dma = pltpu.VMEM, pltpu.SemaphoreType.DMA
    both = [
        vm((NA, 2, 128, cw), BF), vm((NA, 2, 128, cw), BF),
        vm((NA, 2, 2, 128, cw), BF), vm((NA, 2, 2, 128, cw), BF),
        vm((NA, 128, cw), BF), vm((NA, 128, cw), BF),
        vm((NB, 4, 128, cw), BF), vm((NB, 4, 128, cw), BF),
        vm((NB, 2, 64, cw), BF), vm((NB, 2, 64, cw), BF),
        vm((NB, 2, 2, 64, cw), BF), vm((NB, 2, 2, 64, cw), BF),
        vm((CHUNKS, 2, 64, hw), BF), vm((2, 64, hw * CHUNKS), BF),
    ]
    sems = [
        dma((6,)), dma((16,)), dma((16,)), dma((8,)), dma((8,)), dma((8,)), dma((8,)),
        dma((CHUNKS,)), dma((CHUNKS,)), dma((n_t,)), dma((n_t,)), dma((n_t,)), dma((n_t,)), dma, dma, dma((CHUNKS,)), dma((CHUNKS,)),
        dma((NA, 2)), dma((NA, 2)), dma((NA, 2, 2)), dma((NA, 2, 2)), dma((NA,)), dma((NA,)),
        dma((NB, 4)), dma((NB, 4)), dma((NB, 2)), dma((NB, 2)), dma((NB, 2, 2)), dma((NB, 2, 2)),
        dma((CHUNKS,)), dma((CHUNKS,)),
    ]
    hidden = pl.pallas_call(
        kernel,
        out_shape=jax.ShapeDtypeStruct((rows, units), BF),
        in_specs=[pl.BlockSpec(memory_space=pl.ANY)]
        + [pl.BlockSpec(memory_space=pltpu.VMEM)] * 2
        + [pl.BlockSpec(memory_space=pl.ANY)] * 3,
        out_specs=pl.BlockSpec(memory_space=pltpu.VMEM),
        scratch_shapes=[
            vm((rows, kt), BF), vm((16, capacity, kt + 128), BF), vm((256, 2 * ut.shape[0]), BF),
            vm((16 * rows, kc + 256), BF), vm((CHUNKS, kc + 256, cw), BF),
            vm((kc, 2, units // 2), BF), vm(ut.shape, BF), vm(adown.shape, BF), vm((16, capacity, kt + 128), BF),
            vm((n_t, sub, 128), F32), vm((n_t, sub, 128), F32), vm((n_t, sub, 128), BF),
            vm((2, 8, 128), F32), vm((2, CHUNKS, 128, cw), BF), vm((CHUNKS, 16 * rows, cw), F32),
        ] + both + sems,
        compiler_params=pltpu.CompilerParams(
            collective_id=0, has_side_effects=True, vmem_limit_bytes=67043328
        ),
    )(requests, request_adapter.reshape(1, rows), adapter_position.reshape(1, -1), base, ut, adown)
    live = row_index < counts[group]
    return jnp.where(live[:, None], hidden, jnp.zeros_like(hidden))


def solution(mesh):
    placed = (
        P("dp", None),
        P("dp", None, "tensor"),
        P("dp", "tensor", None),
        P("dp", None, None, "tensor"),
        P("dp"),
        P(),
        P(),
    )
    return jax.shard_map(
        body, mesh=mesh, in_specs=placed, out_specs=P("dp", "tensor"), check_vma=False
    )
```
